32 devices in a mesh: real: 2 (over x), tile: 16 (over z, y, core).
Axes of the slice: x: 2, y: 2, z: 4, core: 2. Of those that a mesh axis runs over, the one named last changes fastest.
Arguments:
- positions: float32 [6, 8192], P('real', 'tile'), parts along dimension 0, may hold values from -1.5 to 125.5, as said below
- residual: float32 [6, 8192], P('real', 'tile'), parts along dimension 0, may hold values from -24 to 24
- iterate: float32 [6, 8192], P('real', 'tile'), parts along dimension 0, may hold values from -6 to 6
Outputs:
- new_iterate: float32 [6, 8192], P('real', 'tile'), parts along dimension 0
- new_residual: float32 [6, 8192], P('real', 'tile'), parts along dimension 0
- new_direction: float32 [6, 8192], P('real', 'tile'), parts along dimension 0
The draws below stay inside these ranges and needn't reach their ends.
There are 2 independent parts, one for each index of `real`. The reference program is written for one: setup_inputs(seed, part) draws one part's arguments, and reference() takes and returns one part's arrays. A program takes and returns all parts, laid end to end along the dimension named above; each array names one. Nothing has to cross between parts.
Inputs may be any that keep to these rules, and one draw needn't show every extreme that they name: `positions`: distinct blobs are at least 1 apart.
All inputs are finite; a program needn't handle non-finite values.
Results may differ from the reference program's by a relative error of at most 0.0003.
Values sent between devices are 32-bit elements; how exact they have to be, the bound alone decides.
No kernel may reach another device: no remote copies, remote signals or barrier semaphores. Data moves between devices by JAX's collectives and lax.ppermute only.
A program may use at most 64 MiB of HBM per device.

```python
import math
import jax
import jax.numpy as jnp
from jax import lax

BLOB_DEV = 512
BLOBS = 8192


def lattice_coords(key):
    lattice_site = jax.random.permutation(jax.random.fold_in(key, 5), BLOBS).astype(jnp.int32)
    return jnp.stack([lattice_site % 32, lattice_site // 32 % 32, lattice_site // 1024]).astype(jnp.float32) * 4.0


def smooth_flow(key, strength):
    coords = lattice_coords(key) + 2.0
    layers = (BLOBS + 1023) // 1024
    extent = jnp.array([128.0, 128.0, 4.0 * layers], jnp.float32)[:, None]
    modes = jax.random.randint(jax.random.fold_in(key, 31), (3,), 1, 3).astype(jnp.float32)[:, None]
    flip = jax.random.randint(jax.random.fold_in(key, 32), (), 0, 2).astype(jnp.float32) * 2.0 - 1.0
    rate = math.pi * modes / extent
    phase = rate * coords
    sines = jnp.sin(phase)
    cosines = jnp.cos(phase)
    first = rate[0] * cosines[0] * sines[1] * sines[2]
    second = rate[1] * sines[0] * cosines[1] * sines[2]
    third = rate[2] * sines[0] * sines[1] * cosines[2]
    length = jnp.sqrt(jnp.sum(rate * rate))
    return flip * strength * jnp.stack([first, second, third]) / length


def draw_positions(key, part):
    lattice = lattice_coords(key)
    jitter = jnp.clip(0.6 * jax.random.normal(jax.random.fold_in(key, 11), (3, BLOBS), jnp.float32), -1.5, 1.5)
    return lattice + jitter


def draw_residual(key, part):
    number = jnp.arange(BLOBS, dtype=jnp.int32).astype(jnp.float32)
    growth = 1.0 + 2.0 * number / (BLOBS - 1)
    normal_part = jnp.clip(jax.random.normal(jax.random.fold_in(key, 21), (3, BLOBS), jnp.float32), -3.3, 3.3)
    row_scale = jnp.exp(jax.random.uniform(jax.random.fold_in(key, 22), (3, BLOBS), jnp.float32, 0.0, math.log(10.0)))
    return 0.2 * normal_part * row_scale * growth[None, :] + smooth_flow(key, 2.0)


def steps_of(stream_key, shape, cuts, low, high):
    factor_of, own = 1.0, jax.random.fold_in(stream_key, 6)
    for position, parts in cuts:
        draws = jnp.exp(jax.random.uniform(jax.random.fold_in(own, position), (parts,), jnp.float32, low / len(cuts), high / len(cuts)))
        factor_of = factor_of * jnp.repeat(draws, shape[position] // parts).reshape([-1 if axis == position else 1 for axis in range(len(shape))])
    return factor_of


def bell_draw(rng, shape, width, bound, split=(), held_as=jnp.bfloat16):
    entries = width * jax.random.normal(rng, shape, jnp.float32)
    if split:
        entries = entries * steps_of(rng, shape, split, -0.22, 0.18)
    return jnp.clip(entries, -bound, bound).astype(held_as)


def setup_inputs(seed: int = 0, part: int = 0) -> dict:
    keys = jax.random.split(jax.random.key(seed), 4)
    own_keys = jax.random.split(jax.random.fold_in(keys[3], part), 4)
    positions = draw_positions(jax.random.fold_in(jax.random.fold_in(keys[3], part), 71), part)
    residual = draw_residual(jax.random.fold_in(jax.random.fold_in(keys[3], part), 71), part)
    iterate = bell_draw(own_keys[2], (3, BLOBS), 1.0, 6.0, ((1, 16),), jnp.float32)
    return dict(positions=positions, residual=residual, iterate=iterate)


def pair_terms(row_pos, col_pos):
    separation = row_pos[:, :, None] - col_pos[:, None, :]
    squared = lax.optimization_barrier(jnp.sum(separation * separation, axis=0))
    radius = jnp.sqrt(squared)
    inverse = 1.0 / jnp.maximum(radius, 0.5)
    inverse_sq = inverse * inverse
    far_scalar = 0.75 * inverse * (1.0 + 2.0 / 3.0 * inverse_sq)
    far_tensor = 0.75 * (1.0 - 2.0 * inverse_sq) * inverse_sq * inverse
    touching = radius < 2.0
    scalar_part = jnp.where(touching, 1.0 - 9.0 / 32.0 * radius, far_scalar)
    tensor_part = jnp.where(touching, 3.0 / 32.0 * inverse, far_tensor)
    return (separation, scalar_part, tensor_part)

def toward_rows(separation, scalar_part, tensor_part, col_forces):
    projected = lax.optimization_barrier(jnp.sum(separation * col_forces[:, None, :], axis=0))
    return lax.optimization_barrier(jnp.sum(scalar_part[None] * col_forces[:, None, :] + (tensor_part * projected)[None] * separation, axis=2))

def reference(positions, residual, iterate):
    row_block = 256 if BLOBS % 256 == 0 else BLOB_DEV
    block_count = BLOBS // row_block
    stacked = positions.reshape(3, block_count, row_block).transpose(1, 0, 2)

    def block_image(row_pos):
        separation, scalar_part, tensor_part = pair_terms(row_pos, positions)
        return toward_rows(separation, scalar_part, tensor_part, residual)
    applied = lax.map(block_image, stacked).transpose(1, 0, 2).reshape(3, BLOBS)
    old_norm = jnp.sum(residual * residual)
    curvature = jnp.sum(residual * applied)
    step_size = old_norm / curvature
    new_iterate = iterate + step_size * residual
    new_residual = residual - step_size * applied
    new_norm = jnp.sum(new_residual * new_residual)
    new_direction = new_residual + new_norm / old_norm * residual
    return (new_iterate, new_residual, new_direction)
```

```python
import functools

import jax
import jax.numpy as jnp
from jax import lax
from jax.experimental import pallas as pl
from jax.experimental.pallas import tpu as pltpu
from jax.sharding import PartitionSpec as P

LANES = 128
ROWS = 8


def pair_kernel(diagonal, rows_ref, blobs_ref, base_ref, out_ref):
    cols = blobs_ref.shape[1] // LANES
    own = rows_ref.shape[1]

    def row_tile(tile, carry):
        at = pl.ds(pl.multiple_of(tile * ROWS, ROWS), ROWS)
        px, py, pz = rows_ref[0, at, :], rows_ref[1, at, :], rows_ref[2, at, :]

        def col_tile(col, acc):
            lane = pl.ds(pl.multiple_of(col * LANES, LANES), LANES)
            qx, qy, qz = blobs_ref[0:1, lane], blobs_ref[1:2, lane], blobs_ref[2:3, lane]
            fx, fy, fz = blobs_ref[4:5, lane], blobs_ref[5:6, lane], blobs_ref[6:7, lane]
            dx, dy, dz = px - qx, py - qy, pz - qz
            squared = dx * dx + dy * dy + dz * dz
            if diagonal:
                inverse = lax.rsqrt(jnp.maximum(squared, 0.25))
            else:
                inverse = lax.rsqrt(squared)
            radius = squared * inverse
            inverse_sq = inverse * inverse
            cube = inverse * inverse_sq
            touching = squared < 4.0
            scalar = jnp.where(touching, 1.0 - (9.0 / 32.0) * radius, 0.75 * inverse + 0.5 * cube)
            tensor = jnp.where(touching, (3.0 / 32.0) * inverse, cube * (0.75 - 1.5 * inverse_sq))
            weight = tensor * (dx * fx + dy * fy + dz * fz)
            ax, ay, az = acc
            return (
                ax + (scalar * fx + weight * dx),
                ay + (scalar * fy + weight * dy),
                az + (scalar * fz + weight * dz),
            )

        acc = tuple(base_ref[k, at, :] for k in range(3))
        acc = lax.fori_loop(0, cols, col_tile, acc, unroll=4)
        for k in range(3):
            out_ref[k, at, :] = acc[k]
        return carry

    lax.fori_loop(0, own // ROWS, row_tile, 0)


def add_pairs(diagonal, rows, blobs, base):
    own = rows.shape[1]
    pairs = own * blobs.shape[1]
    return pl.pallas_call(
        functools.partial(pair_kernel, diagonal),
        out_shape=jax.ShapeDtypeStruct(base.shape, jnp.float32),
        in_specs=[pl.BlockSpec(memory_space=pltpu.VMEM)] * 3,
        out_specs=pl.BlockSpec(memory_space=pltpu.VMEM),
        input_output_aliases={2: 0},
        compiler_params=pltpu.CompilerParams(vmem_limit_bytes=4 << 20),
        cost_estimate=pl.CostEstimate(flops=45 * pairs, bytes_accessed=4 * 2 * base.size, transcendentals=pairs),
    )(rows, blobs, base)


def strides(devices):
    out, step = [], devices // 2
    while step:
        out.append(step)
        step //= 2
    return out


def swap(value, devices, step):
    return lax.ppermute(value, "tile", [(i, i ^ step) for i in range(devices)])


def shards(devices, positions, residual, iterate):
    own = positions.shape[1]
    gap = jnp.zeros((1, own), jnp.float32)
    held = jnp.concatenate([positions, gap, residual, gap], axis=0)
    rows = jnp.broadcast_to(positions[:, :, None], (3, own, LANES))
    applied = jnp.zeros((3, own, LANES), jnp.float32)
    fresh, diagonal = held, True
    for step in strides(devices):
        arrived = swap(held, devices, step)
        applied = add_pairs(diagonal, rows, fresh, applied)
        applied, arrived = lax.optimization_barrier((applied, arrived))
        held = jnp.concatenate([held, arrived], axis=1)
        fresh, diagonal = arrived, False
    applied = add_pairs(diagonal, rows, fresh, applied)
    image = jnp.sum(applied, axis=2)
    sums = jnp.stack([jnp.sum(residual * residual), jnp.sum(residual * image), jnp.sum(image * image)])
    for step in strides(devices):
        sums = sums + swap(sums, devices, step)
    old_norm, curvature, image_norm = sums[0], sums[1], sums[2]
    step_size = old_norm / curvature
    new_norm = old_norm - 2.0 * step_size * curvature + step_size * step_size * image_norm
    new_residual = residual - step_size * image
    new_iterate = iterate + step_size * residual
    new_direction = new_residual + new_norm / old_norm * residual
    return (new_iterate, new_residual, new_direction)


def solution(mesh):
    spec = P("real", "tile")
    return jax.shard_map(
        functools.partial(shards, mesh.shape["tile"]),
        mesh=mesh,
        in_specs=(spec, spec, spec),
        out_specs=(spec, spec, spec),
        check_vma=False,
    )
```

```python
import functools

import jax
import jax.numpy as jnp
from jax import lax
from jax.experimental import pallas as pl
from jax.experimental.pallas import tpu as pltpu
from jax.sharding import PartitionSpec as P

LANES = 128
ROWS = 8
SUB = 128
DEPTH = 128
CENTRE = 64.0
STRETCH = 1.5**0.5
FORCE = 0.75 * STRETCH
NEAR_SQ = 4.0 * 1.5
NEAR_CONST = 1.0 / FORCE
NEAR_SLOPE = 9.0 / (32.0 * STRETCH * FORCE)
NEAR_TENSOR = 1.0 / 36.0
FAR_AWAY = 1e30


def bf16(value):
    return value.astype(jnp.bfloat16).astype(jnp.float32)


def thirds(value):
    high = bf16(value)
    rest = value - high
    middle = bf16(rest)
    return high, middle, bf16(rest - middle)


def row_index(value):
    return lax.broadcasted_iota(jnp.int32, value.shape, 0)


def splits(blobs):
    row = row_index(blobs)
    place = row < 4
    tripled = jnp.where((row >= 4) & (row < 7), 3.0 * blobs, blobs)
    high = jnp.where(place, 0.5 * jnp.round(2.0 * blobs), bf16(tripled))
    rest = tripled - high
    middle = bf16(rest)
    low = bf16(rest - middle)
    return tripled, high, rest, middle, low


def column_features(blobs):
    row = row_index(blobs)
    tripled, high, rest, middle, low = splits(blobs)
    product = jnp.where(row < 4, high * high, tripled * pltpu.roll(blobs, 4, 0))
    p_high, p_middle, p_low = thirds(product)
    e_high, e_middle, e_low = thirds(rest * (2.0 * high + rest))
    zero = jnp.zeros_like(blobs)
    return [
        high, p_high, p_middle, high, high, middle, middle, middle,
        low, low, p_low, e_high, e_middle, e_low, zero, zero,
    ]


def row_features(blobs):
    row = row_index(blobs)
    place = row < 3
    _, high, rest, middle, low = splits(blobs)
    n_high, n_middle, n_low = thirds(jnp.sum(jnp.where(place, high * high, 0.0), axis=0, keepdims=True))
    fine = rest * (2.0 * high + rest)
    m_high, m_middle, m_low = thirds(jnp.sum(jnp.where(place, fine, 0.0), axis=0, keepdims=True))
    zero = jnp.zeros_like(blobs)
    one = jnp.where(place, 1.0, zero)

    def on(base, third, seventh):
        base = jnp.where(row == 3, third, jnp.where(place, base, 0.0))
        return jnp.where(row == 7, seventh, base)

    far = [
        on(-2.0 * high, n_high, n_middle), on(one, n_low, 0.0), one,
        on(-2.0 * middle, m_high, m_middle), on(-2.0 * low, m_low, 0.0),
        on(-2.0 * high, 0.0, 0.0), on(-2.0 * middle, 0.0, 0.0), on(-2.0 * low, 0.0, 0.0),
        on(-2.0 * high, 0.0, 0.0), on(-2.0 * middle, 0.0, 0.0),
        zero, one, one, one, zero, zero,
    ]

    def lift(value):
        return pltpu.roll(jnp.where(place, value, 0.0), 4, 0)

    big, mid, small, minus = lift(high), lift(middle), lift(low), lift(-one)
    along = [
        big, minus, minus, mid, small, big, mid, small,
        big, mid, minus, zero, zero, zero, zero, zero,
    ]
    return far, along


def pair_kernel(diagonal, *refs):
    if diagonal:
        blobs_ref, out_ref, lhs_ref, rhs_ref, even_ref, odd_ref = refs
    else:
        blobs_ref, lhs_ref, base_ref, out_ref, rhs_ref, even_ref, odd_ref = refs
    subs = lhs_ref.shape[0]
    own = subs * SUB
    chunks = blobs_ref.shape[1] // own
    steps = subs * chunks

    if diagonal:
        far, along = row_features(blobs_ref[...])
        far = jnp.concatenate(far, axis=0).T.astype(jnp.bfloat16)
        along = jnp.concatenate(along, axis=0).T.astype(jnp.bfloat16)
        for sub in range(subs):
            lhs_ref[sub, :SUB, :] = far[sub * SUB : (sub + 1) * SUB]
            lhs_ref[sub, SUB:, :] = along[sub * SUB : (sub + 1) * SUB]

    def features(chunk, carry):
        lanes = pl.ds(pl.multiple_of(chunk * own, own), own)
        groups = column_features(blobs_ref[:, lanes])
        for pair in range(DEPTH // 16):
            both = jnp.concatenate(groups[2 * pair : 2 * pair + 2], axis=0)
            rhs_ref[16 * pair : 16 * pair + 16, lanes] = both.astype(jnp.bfloat16)
        return carry

    lax.fori_loop(0, chunks, features, 0)

    def products(step, into_ref):
        lanes = pl.ds(pl.multiple_of(step // subs * own, own), own)
        into_ref[...] = jnp.dot(lhs_ref[step % subs], rhs_ref[:, lanes], preferred_element_type=jnp.float32)

    def add_step(step, from_ref):
        first_row = pl.multiple_of(step % subs * SUB, SUB)
        first_lane = pl.multiple_of(step // subs * own, own)
        source = out_ref if diagonal else None
        columns = []
        for col in range(own // LANES):
            lanes = pl.ds(first_lane + col * LANES, LANES)
            columns.append([jnp.broadcast_to(blobs_ref[k : k + 1, lanes], (ROWS, LANES)) for k in (0, 1, 2, 4, 5, 6)])
        for tile in range(SUB // ROWS):
            at = pl.ds(first_row + tile * ROWS, ROWS)
            acc = [out_ref[k, at, :] for k in range(4)]
            for col in range(own // LANES):
                here = slice(tile * ROWS, (tile + 1) * ROWS)
                there = slice(SUB + tile * ROWS, SUB + (tile + 1) * ROWS)
                lanes = slice(col * LANES, (col + 1) * LANES)
                squared, projected = from_ref[here, lanes], from_ref[there, lanes]
                if diagonal:
                    i = lax.broadcasted_iota(jnp.int32, (ROWS, LANES), 0) + (first_row + tile * ROWS)
                    j = lax.broadcasted_iota(jnp.int32, (ROWS, LANES), 1) + col * LANES
                    squared = jnp.where(i == j, FAR_AWAY, squared)
                inverse = lax.rsqrt(squared)
                inverse_sq = inverse * inverse
                cube = inverse * inverse_sq
                near = squared < NEAR_SQ
                scalar = jnp.where(near, NEAR_CONST - NEAR_SLOPE * (squared * inverse), inverse + cube)
                tensor = jnp.where(near, NEAR_TENSOR * inverse, cube * (1.0 / 3.0 - inverse_sq))
                weight = tensor * projected
                x, y, z, fx, fy, fz = columns[col]
                acc[0] = acc[0] + (scalar * fx - weight * x)
                acc[1] = acc[1] + (scalar * fy - weight * y)
                acc[2] = acc[2] + (scalar * fz - weight * z)
                acc[3] = acc[3] + weight
            for k in range(4):
                out_ref[k, at, :] = acc[k]

    out_ref[...] = jnp.zeros_like(out_ref) if diagonal else base_ref[...]
    products(0, even_ref)

    def two_steps(turn, carry):
        step = 2 * turn
        products(step + 1, odd_ref)
        add_step(step, even_ref)
        products(jnp.minimum(step + 2, steps - 1), even_ref)
        add_step(step + 1, odd_ref)
        return carry

    lax.fori_loop(0, steps // 2, two_steps, 0)


def pair_call(blobs, lhs=None, base=None):
    diagonal = lhs is None
    own = blobs.shape[1] if diagonal else lhs.shape[0] * SUB
    vmem = pl.BlockSpec(memory_space=pltpu.VMEM)
    sums = jax.ShapeDtypeStruct((4, own, LANES), jnp.float32)
    rows = jax.ShapeDtypeStruct((own // SUB, 2 * SUB, DEPTH), jnp.bfloat16)
    pairs = own * blobs.shape[1]
    return pl.pallas_call(
        functools.partial(pair_kernel, diagonal),
        out_shape=(sums, rows) if diagonal else sums,
        in_specs=[vmem] * (1 if diagonal else 3),
        out_specs=(vmem, vmem) if diagonal else vmem,
        scratch_shapes=[
            pltpu.VMEM((DEPTH, blobs.shape[1]), jnp.bfloat16),
            pltpu.VMEM((2 * SUB, own), jnp.float32),
            pltpu.VMEM((2 * SUB, own), jnp.float32),
        ],
        input_output_aliases={} if diagonal else {2: 0},
        compiler_params=pltpu.CompilerParams(vmem_limit_bytes=16 << 20),
        cost_estimate=pl.CostEstimate(flops=45 * pairs, bytes_accessed=32 * blobs.shape[1], transcendentals=pairs),
    )(*([blobs] if diagonal else [blobs, lhs, base]))


def finish_kernel(sums_ref, blobs_ref, residual_ref, image_ref, norms_ref):
    ones = jnp.ones((ROWS, LANES), jnp.float32)

    def total(k):
        added = lax.dot_general(
            ones, sums_ref[k], (((1,), (1,)), ((), ())), precision=lax.Precision.HIGHEST, preferred_element_type=jnp.float32
        )
        return added[0:1, :]

    weight = total(3)
    for k in range(3):
        image_ref[k : k + 1, :] = residual_ref[k : k + 1, :] + (total(k) + weight * blobs_ref[k : k + 1, :])
    image, residual = image_ref[...], residual_ref[...]

    def fold(value):
        value = jnp.sum(value, axis=0, keepdims=True)
        return sum(value[:, lane : lane + LANES] for lane in range(0, value.shape[1], LANES))

    norms_ref[...] = jnp.zeros_like(norms_ref)
    norms_ref[0:1, :] = fold(residual * residual)
    norms_ref[1:2, :] = fold(residual * image)
    norms_ref[2:3, :] = fold(image * image)


def finish(sums, blobs, residual):
    vmem = pl.BlockSpec(memory_space=pltpu.VMEM)
    return pl.pallas_call(
        finish_kernel,
        out_shape=(jax.ShapeDtypeStruct(residual.shape, jnp.float32), jax.ShapeDtypeStruct((ROWS, LANES), jnp.float32)),
        in_specs=[vmem] * 3,
        out_specs=(vmem, vmem),
        compiler_params=pltpu.CompilerParams(vmem_limit_bytes=8 << 20),
    )(sums, blobs, residual)


def update_kernel(mine_ref, other_ref, image_ref, residual_ref, iterate_ref, new_iterate_ref, new_residual_ref, new_direction_ref):
    norms = jnp.sum(mine_ref[...] + other_ref[...], axis=1, keepdims=True)
    old_norm, curvature, image_norm = norms[0:1], norms[1:2], norms[2:3]
    step_size = old_norm / curvature
    new_norm = old_norm - 2.0 * step_size * curvature + step_size * step_size * image_norm
    residual = residual_ref[...]
    new_residual = residual - step_size * image_ref[...]
    new_iterate_ref[...] = iterate_ref[...] + step_size * residual
    new_residual_ref[...] = new_residual
    new_direction_ref[...] = new_residual + new_norm / old_norm * residual


def update(mine, other, image, residual, iterate):
    vmem = pl.BlockSpec(memory_space=pltpu.VMEM)
    shape = jax.ShapeDtypeStruct(residual.shape, jnp.float32)
    return pl.pallas_call(
        update_kernel,
        out_shape=(shape,) * 3,
        in_specs=[vmem] * 5,
        out_specs=(vmem,) * 3,
        compiler_params=pltpu.CompilerParams(vmem_limit_bytes=4 << 20),
    )(mine, other, image, residual, iterate)


def strides(devices):
    out, step = [], devices // 2
    while step:
        out.append(step)
        step //= 2
    return out


def swap(value, devices, step):
    return lax.ppermute(value, "tile", [(i, i ^ step) for i in range(devices)])


def shards(devices, positions, residual, iterate):
    one = jnp.ones((1, positions.shape[1]), jnp.float32)
    blobs = jnp.concatenate([STRETCH * (positions - CENTRE), one, FORCE * residual, one], axis=0)
    held, fresh, sums, lhs = blobs, blobs, None, None
    for step in strides(devices):
        arrived = swap(held, devices, step)
        if lhs is None:
            sums, lhs = pair_call(fresh)
        else:
            sums = pair_call(fresh, lhs, sums)
        sums, arrived = lax.optimization_barrier((sums, arrived))
        held = jnp.concatenate([held, arrived], axis=1)
        fresh = arrived
    sums = pair_call(fresh, lhs, sums)
    image, norms = finish(sums, blobs, residual)
    other = jnp.zeros_like(norms)
    for step in strides(devices):
        norms = norms + other
        other = swap(norms, devices, step)
    return update(norms, other, image, residual, iterate)


def solution(mesh):
    spec = P("real", "tile")
    return jax.shard_map(
        functools.partial(shards, mesh.shape["tile"]),
        mesh=mesh,
        in_specs=(spec, spec, spec),
        out_specs=(spec, spec, spec),
        check_vma=False,
    )
```

```python
import functools

import jax
import jax.numpy as jnp
from jax import lax
from jax.experimental import pallas as pl
from jax.experimental.pallas import tpu as pltpu
from jax.sharding import PartitionSpec as P

LANES = 128
ROWS = 8
PIECE = 512
DEPTH = 128
CENTRE = 64.0
STRETCH = 1.5**0.5
FORCE = 0.75 * STRETCH
NEAR_SQ = 4.0 * 1.5
NEAR_CONST = 1.0 / FORCE
NEAR_SLOPE = 9.0 / (32.0 * STRETCH * FORCE)
NEAR_TENSOR = 1.0 / 36.0
FAR_AWAY = 1e30


def bf16(value):
    return value.astype(jnp.bfloat16).astype(jnp.float32)


def thirds(value):
    high = bf16(value)
    rest = value - high
    middle = bf16(rest)
    return high, middle, bf16(rest - middle)


def row_index(value):
    return lax.broadcasted_iota(jnp.int32, value.shape, 0)


def splits(blobs):
    row = row_index(blobs)
    place = row < 4
    tripled = jnp.where((row >= 4) & (row < 7), 3.0 * blobs, blobs)
    high = jnp.where(place, 0.5 * jnp.round(2.0 * blobs), bf16(tripled))
    rest = tripled - high
    middle = bf16(rest)
    low = bf16(rest - middle)
    return tripled, high, rest, middle, low


def column_features(blobs):
    row = row_index(blobs)
    tripled, high, rest, middle, low = splits(blobs)
    product = jnp.where(row < 4, high * high, tripled * pltpu.roll(blobs, 4, 0))
    p_high, p_middle, p_low = thirds(product)
    e_high, e_middle, e_low = thirds(rest * (2.0 * high + rest))
    zero = jnp.zeros_like(blobs)
    return [
        high, p_high, p_middle, high, high, middle, middle, middle,
        low, low, p_low, e_high, e_middle, e_low, zero, zero,
    ]


def row_features(blobs):
    row = row_index(blobs)
    place = row < 3
    _, high, rest, middle, low = splits(blobs)
    n_high, n_middle, n_low = thirds(jnp.sum(jnp.where(place, high * high, 0.0), axis=0, keepdims=True))
    fine = rest * (2.0 * high + rest)
    m_high, m_middle, m_low = thirds(jnp.sum(jnp.where(place, fine, 0.0), axis=0, keepdims=True))
    zero = jnp.zeros_like(blobs)
    one = jnp.where(place, 1.0, zero)

    def on(base, third, seventh):
        base = jnp.where(row == 3, third, jnp.where(place, base, 0.0))
        return jnp.where(row == 7, seventh, base)

    far = [
        on(-2.0 * high, n_high, n_middle), on(one, n_low, 0.0), one,
        on(-2.0 * middle, m_high, m_middle), on(-2.0 * low, m_low, 0.0),
        on(-2.0 * high, 0.0, 0.0), on(-2.0 * middle, 0.0, 0.0), on(-2.0 * low, 0.0, 0.0),
        on(-2.0 * high, 0.0, 0.0), on(-2.0 * middle, 0.0, 0.0),
        zero, one, one, one, zero, zero,
    ]

    def lift(value):
        return pltpu.roll(jnp.where(place, value, 0.0), 4, 0)

    big, mid, small, minus = lift(high), lift(middle), lift(low), lift(-one)
    along = [
        big, minus, minus, mid, small, big, mid, small,
        big, mid, minus, zero, zero, zero, zero, zero,
    ]
    return far, along


def pair_kernel(diagonal, *refs):
    if diagonal:
        blobs_ref, out_ref, lhs_ref, rhs_ref, *products_refs = refs
    else:
        blobs_ref, lhs_ref, base_ref, out_ref, rhs_ref, *products_refs = refs
    own = lhs_ref.shape[1]
    cols = blobs_ref.shape[1] // LANES
    sub = products_refs[0].shape[0] // 2
    steps = own // sub

    if diagonal:
        far, along = row_features(blobs_ref[...])
        lhs_ref[0] = jnp.concatenate(far, axis=0).T.astype(jnp.bfloat16)
        lhs_ref[1] = jnp.concatenate(along, axis=0).T.astype(jnp.bfloat16)

    def features(chunk, carry):
        lanes = pl.ds(pl.multiple_of(chunk * own, own), own)
        groups = column_features(blobs_ref[:, lanes])
        for pair in range(DEPTH // 16):
            both = jnp.concatenate(groups[2 * pair : 2 * pair + 2], axis=0)
            rhs_ref[16 * pair : 16 * pair + 16, lanes] = both.astype(jnp.bfloat16)
        return carry

    lax.fori_loop(0, blobs_ref.shape[1] // own, features, 0)

    def products(step, piece):
        rows = pl.ds(pl.multiple_of(step * sub, sub), sub)
        lanes = slice(piece * PIECE, (piece + 1) * PIECE)
        both = jnp.concatenate([lhs_ref[0, rows, :], lhs_ref[1, rows, :]], axis=0)
        products_refs[piece][...] = jnp.dot(both, rhs_ref[:, lanes], preferred_element_type=jnp.float32)

    def add_column(step, col, acc):
        first_row = pl.multiple_of(step * sub, sub)
        products_ref = products_refs[col * LANES // PIECE]
        there = slice(col * LANES % PIECE, col * LANES % PIECE + LANES)
        lanes = slice(col * LANES, (col + 1) * LANES)
        x, y, z, fx, fy, fz = (
            jnp.broadcast_to(blobs_ref[k : k + 1, lanes], (ROWS, LANES)) for k in (0, 1, 2, 4, 5, 6)
        )
        for tile, mine in enumerate(acc):
            squared = products_ref[tile * ROWS : (tile + 1) * ROWS, there]
            projected = products_ref[sub + tile * ROWS : sub + (tile + 1) * ROWS, there]
            if diagonal:
                i = lax.broadcasted_iota(jnp.int32, (ROWS, LANES), 0) + (first_row + tile * ROWS)
                j = lax.broadcasted_iota(jnp.int32, (ROWS, LANES), 1) + col * LANES
                squared = jnp.where(i == j, FAR_AWAY, squared)
            inverse = lax.rsqrt(squared)
            limited = jnp.minimum(inverse * inverse, 1.0 / NEAR_SQ)
            cube = inverse * limited
            near_scalar = NEAR_CONST - NEAR_SLOPE * (squared * inverse)
            scalar = jnp.where(squared < NEAR_SQ, near_scalar, inverse + cube)
            weight = cube * (1.0 / 3.0 - limited) * projected
            mine[0] = mine[0] + (scalar * fx - weight * x)
            mine[1] = mine[1] + (scalar * fy - weight * y)
            mine[2] = mine[2] + (scalar * fz - weight * z)
            mine[3] = mine[3] + weight

    pieces = cols * LANES // PIECE
    for piece in range(pieces):
        products(0, piece)

    def add_step(step, carry):
        later = jnp.minimum(step + 1, steps - 1)
        rows = [pl.ds(pl.multiple_of(step * sub, sub) + tile * ROWS, ROWS) for tile in range(sub // ROWS)]
        if diagonal:
            acc = [[jnp.zeros((ROWS, LANES), jnp.float32) for k in range(4)] for _ in rows]
        else:
            acc = [[base_ref[k, row, :] for k in range(4)] for row in rows]
        for group in range(pieces):
            for col in range(group * PIECE // LANES, (group + 1) * PIECE // LANES):
                add_column(step, col, acc)
            products(later, group)
        for row, mine in zip(rows, acc):
            for k in range(4):
                out_ref[k, row, :] = mine[k]
        return carry

    lax.fori_loop(0, steps, add_step, 0)


def pair_call(blobs, lhs=None, base=None):
    diagonal = lhs is None
    wide = blobs.shape[1]
    own = wide if diagonal else lhs.shape[1]
    sub = max(64, 128 * 512 // wide)
    vmem = pl.BlockSpec(memory_space=pltpu.VMEM)
    sums = jax.ShapeDtypeStruct((4, own, LANES), jnp.float32)
    rows = jax.ShapeDtypeStruct((2, own, DEPTH), jnp.bfloat16)
    pairs = own * wide
    return pl.pallas_call(
        functools.partial(pair_kernel, diagonal),
        out_shape=(sums, rows) if diagonal else sums,
        in_specs=[vmem] * (1 if diagonal else 3),
        out_specs=(vmem, vmem) if diagonal else vmem,
        scratch_shapes=[
            pltpu.VMEM((DEPTH, wide), jnp.bfloat16),
        ]
        + [pltpu.VMEM((2 * sub, PIECE), jnp.float32)] * (wide // PIECE),
        input_output_aliases={} if diagonal else {2: 0},
        compiler_params=pltpu.CompilerParams(vmem_limit_bytes=16 << 20),
        cost_estimate=pl.CostEstimate(flops=45 * pairs, bytes_accessed=32 * wide, transcendentals=pairs),
    )(*([blobs] if diagonal else [blobs, lhs, base]))


WIDEST = 4096


def add_pairs(blobs, lhs, sums):
    for first in range(0, blobs.shape[1], WIDEST):
        sums = pair_call(blobs[:, first : first + WIDEST], lhs, sums)
    return sums


def finish_kernel(sums_ref, blobs_ref, residual_ref, image_ref, norms_ref):
    ones = jnp.ones((ROWS, LANES), jnp.float32)

    def total(k):
        added = lax.dot_general(
            ones, sums_ref[k], (((1,), (1,)), ((), ())), precision=lax.Precision.HIGHEST, preferred_element_type=jnp.float32
        )
        return added[0:1, :]

    weight = total(3)
    for k in range(3):
        image_ref[k : k + 1, :] = residual_ref[k : k + 1, :] + (total(k) + weight * blobs_ref[k : k + 1, :])
    image, residual = image_ref[...], residual_ref[...]

    def fold(value):
        value = jnp.sum(value, axis=0, keepdims=True)
        return sum(value[:, lane : lane + LANES] for lane in range(0, value.shape[1], LANES))

    norms_ref[...] = jnp.zeros_like(norms_ref)
    norms_ref[0:1, :] = fold(residual * residual)
    norms_ref[1:2, :] = fold(residual * image)
    norms_ref[2:3, :] = fold(image * image)


def finish(sums, blobs, residual):
    vmem = pl.BlockSpec(memory_space=pltpu.VMEM)
    return pl.pallas_call(
        finish_kernel,
        out_shape=(jax.ShapeDtypeStruct(residual.shape, jnp.float32), jax.ShapeDtypeStruct((ROWS, LANES), jnp.float32)),
        in_specs=[vmem] * 3,
        out_specs=(vmem, vmem),
        compiler_params=pltpu.CompilerParams(vmem_limit_bytes=8 << 20),
    )(sums, blobs, residual)


def update_kernel(mine_ref, other_ref, image_ref, residual_ref, iterate_ref, new_iterate_ref, new_residual_ref, new_direction_ref):
    norms = jnp.sum(mine_ref[...] + other_ref[...], axis=1, keepdims=True)
    old_norm, curvature, image_norm = norms[0:1], norms[1:2], norms[2:3]
    step_size = old_norm / curvature
    new_norm = old_norm - 2.0 * step_size * curvature + step_size * step_size * image_norm
    residual = residual_ref[...]
    new_residual = residual - step_size * image_ref[...]
    new_iterate_ref[...] = iterate_ref[...] + step_size * residual
    new_residual_ref[...] = new_residual
    new_direction_ref[...] = new_residual + new_norm / old_norm * residual


def update(mine, other, image, residual, iterate):
    vmem = pl.BlockSpec(memory_space=pltpu.VMEM)
    shape = jax.ShapeDtypeStruct(residual.shape, jnp.float32)
    return pl.pallas_call(
        update_kernel,
        out_shape=(shape,) * 3,
        in_specs=[vmem] * 5,
        out_specs=(vmem,) * 3,
        compiler_params=pltpu.CompilerParams(vmem_limit_bytes=4 << 20),
    )(mine, other, image, residual, iterate)


def strides(devices):
    out, step = [], devices // 2
    while step:
        out.append(step)
        step //= 2
    return out


def swap(value, devices, step):
    return lax.ppermute(value, "tile", [(i, i ^ step) for i in range(devices)])


def shards(devices, positions, residual, iterate):
    one = jnp.ones((1, positions.shape[1]), jnp.float32)
    blobs = jnp.concatenate([STRETCH * (positions - CENTRE), one, FORCE * residual, one], axis=0)
    held, fresh, sums, lhs = blobs, blobs, None, None
    for step in strides(devices):
        arrived = swap(held, devices, step)
        if lhs is None:
            sums, lhs = pair_call(fresh)
        else:
            sums = add_pairs(fresh, lhs, sums)
        sums, arrived = lax.optimization_barrier((sums, arrived))
        held = jnp.concatenate([held, arrived], axis=1)
        fresh = arrived
    sums = add_pairs(fresh, lhs, sums)
    image, norms = finish(sums, blobs, residual)
    other = jnp.zeros_like(norms)
    for step in strides(devices):
        norms = norms + other
        other = swap(norms, devices, step)
    return update(norms, other, image, residual, iterate)


def solution(mesh):
    spec = P("real", "tile")
    return jax.shard_map(
        functools.partial(shards, mesh.shape["tile"]),
        mesh=mesh,
        in_specs=(spec, spec, spec),
        out_specs=(spec, spec, spec),
        check_vma=False,
    )
```

```python
import functools

import jax
import jax.numpy as jnp
from jax import lax
from jax.experimental import pallas as pl
from jax.experimental.pallas import tpu as pltpu
from jax.sharding import PartitionSpec as P

LANES = 128
ROWS = 8
PIECE = 512
DEPTH = 128
CENTRE = 64.0
STRETCH = 1.5**0.5
FORCE = 0.75 * STRETCH
NEAR_SQ = 4.0 * 1.5
NEAR_CONST = 1.0 / FORCE
NEAR_SLOPE = 9.0 / (32.0 * STRETCH * FORCE)
NEAR_TENSOR = 1.0 / 36.0
FAR_AWAY = 1e30


def bf16(value):
    return value.astype(jnp.bfloat16).astype(jnp.float32)


def thirds(value):
    high = bf16(value)
    rest = value - high
    middle = bf16(rest)
    return high, middle, bf16(rest - middle)


def row_index(value):
    return lax.broadcasted_iota(jnp.int32, value.shape, 0)


def splits(blobs):
    row = row_index(blobs)
    place = row < 4
    tripled = jnp.where((row >= 4) & (row < 7), 3.0 * blobs, blobs)
    high = jnp.where(place, 0.5 * jnp.round(2.0 * blobs), bf16(tripled))
    rest = tripled - high
    middle = bf16(rest)
    low = bf16(rest - middle)
    return tripled, high, rest, middle, low


def column_features(blobs):
    row = row_index(blobs)
    tripled, high, rest, middle, low = splits(blobs)
    product = jnp.where(row < 4, high * high, tripled * pltpu.roll(blobs, 4, 0))
    p_high, p_middle, p_low = thirds(product)
    e_high, e_middle, e_low = thirds(rest * (2.0 * high + rest))
    zero = jnp.zeros_like(blobs)
    return [
        high, p_high, p_middle, high, high, middle, middle, middle,
        low, low, p_low, e_high, e_middle, e_low, zero, zero,
    ]


def row_features(blobs):
    row = row_index(blobs)
    place = row < 3
    _, high, rest, middle, low = splits(blobs)
    n_high, n_middle, n_low = thirds(jnp.sum(jnp.where(place, high * high, 0.0), axis=0, keepdims=True))
    fine = rest * (2.0 * high + rest)
    m_high, m_middle, m_low = thirds(jnp.sum(jnp.where(place, fine, 0.0), axis=0, keepdims=True))
    zero = jnp.zeros_like(blobs)
    one = jnp.where(place, 1.0, zero)

    def on(base, third, seventh):
        base = jnp.where(row == 3, third, jnp.where(place, base, 0.0))
        return jnp.where(row == 7, seventh, base)

    far = [
        on(-2.0 * high, n_high, n_middle), on(one, n_low, 0.0), one,
        on(-2.0 * middle, m_high, m_middle), on(-2.0 * low, m_low, 0.0),
        on(-2.0 * high, 0.0, 0.0), on(-2.0 * middle, 0.0, 0.0), on(-2.0 * low, 0.0, 0.0),
        on(-2.0 * high, 0.0, 0.0), on(-2.0 * middle, 0.0, 0.0),
        zero, one, one, one, zero, zero,
    ]

    def lift(value):
        return pltpu.roll(jnp.where(place, value, 0.0), 4, 0)

    big, mid, small, minus = lift(high), lift(middle), lift(low), lift(-one)
    along = [
        big, minus, minus, mid, small, big, mid, small,
        big, mid, minus, zero, zero, zero, zero, zero,
    ]
    return far, along


def pair_kernel(diagonal, last, *refs):
    if diagonal:
        blobs_ref, out_ref, lhs_ref, rhs_ref, *products_refs = refs
    elif last:
        blobs_ref, lhs_ref, base_ref, own_ref, residual_ref, image_ref, norms_ref, out_ref, rhs_ref, *products_refs = refs
    else:
        blobs_ref, lhs_ref, base_ref, out_ref, rhs_ref, *products_refs = refs
    own = lhs_ref.shape[1]
    cols = blobs_ref.shape[1] // LANES
    sub = products_refs[0].shape[0] // 2
    steps = own // sub

    if diagonal:
        far, along = row_features(blobs_ref[...])
        lhs_ref[0] = jnp.concatenate(far, axis=0).T.astype(jnp.bfloat16)
        lhs_ref[1] = jnp.concatenate(along, axis=0).T.astype(jnp.bfloat16)

    def features(chunk, carry):
        lanes = pl.ds(pl.multiple_of(chunk * own, own), own)
        groups = column_features(blobs_ref[:, lanes])
        for pair in range(DEPTH // 16):
            both = jnp.concatenate(groups[2 * pair : 2 * pair + 2], axis=0)
            rhs_ref[16 * pair : 16 * pair + 16, lanes] = both.astype(jnp.bfloat16)
        return carry

    lax.fori_loop(0, blobs_ref.shape[1] // own, features, 0)

    def products(step, piece):
        rows = pl.ds(pl.multiple_of(step * sub, sub), sub)
        lanes = slice(piece * PIECE, (piece + 1) * PIECE)
        both = jnp.concatenate([lhs_ref[0, rows, :], lhs_ref[1, rows, :]], axis=0)
        products_refs[piece][...] = jnp.dot(both, rhs_ref[:, lanes], preferred_element_type=jnp.float32)

    def add_column(step, col, acc):
        first_row = pl.multiple_of(step * sub, sub)
        products_ref = products_refs[col * LANES // PIECE]
        there = slice(col * LANES % PIECE, col * LANES % PIECE + LANES)
        lanes = slice(col * LANES, (col + 1) * LANES)
        x, y, z, fx, fy, fz = (
            jnp.broadcast_to(blobs_ref[k : k + 1, lanes], (ROWS, LANES)) for k in (0, 1, 2, 4, 5, 6)
        )
        for tile, mine in enumerate(acc):
            squared = products_ref[tile * ROWS : (tile + 1) * ROWS, there]
            projected = products_ref[sub + tile * ROWS : sub + (tile + 1) * ROWS, there]
            if diagonal:
                i = lax.broadcasted_iota(jnp.int32, (ROWS, LANES), 0) + (first_row + tile * ROWS)
                j = lax.broadcasted_iota(jnp.int32, (ROWS, LANES), 1) + col * LANES
                squared = jnp.where(i == j, FAR_AWAY, squared)
            inverse = lax.rsqrt(squared)
            limited = jnp.minimum(inverse * inverse, 1.0 / NEAR_SQ)
            cube = inverse * limited
            near_scalar = NEAR_CONST - NEAR_SLOPE * (squared * inverse)
            scalar = jnp.where(squared < NEAR_SQ, near_scalar, inverse + cube)
            weight = cube * (1.0 / 3.0 - limited) * projected
            mine[0] = mine[0] + (scalar * fx - weight * x)
            mine[1] = mine[1] + (scalar * fy - weight * y)
            mine[2] = mine[2] + (scalar * fz - weight * z)
            mine[3] = mine[3] + weight

    pieces = cols * LANES // PIECE
    for piece in range(pieces):
        products(0, piece)

    def add_step(step, carry):
        later = jnp.minimum(step + 1, steps - 1)
        rows = [pl.ds(pl.multiple_of(step * sub, sub) + tile * ROWS, ROWS) for tile in range(sub // ROWS)]
        if diagonal:
            acc = [[jnp.zeros((ROWS, LANES), jnp.float32) for k in range(4)] for _ in rows]
        else:
            acc = [[base_ref[k, row, :] for k in range(4)] for row in rows]
        for group in range(pieces):
            for col in range(group * PIECE // LANES, (group + 1) * PIECE // LANES):
                add_column(step, col, acc)
            products(later, group)
        for row, mine in zip(rows, acc):
            for k in range(4):
                out_ref[k, row, :] = mine[k]
        return carry

    lax.fori_loop(0, steps, add_step, 0)

    if last:
        finish(out_ref, own_ref, residual_ref, image_ref, norms_ref)


def finish(sums_ref, own_ref, residual_ref, image_ref, norms_ref):
    row = lax.broadcasted_iota(jnp.int32, (ROWS, LANES), 0)
    lane = lax.broadcasted_iota(jnp.int32, (ROWS, LANES), 1)
    on_row = row == lane % ROWS
    on_tile = lane // ROWS

    def total(k, first):
        spread = jnp.zeros((ROWS, LANES), jnp.float32)
        for tile in range(LANES // ROWS):
            start = first + tile * ROWS
            added = jnp.sum(sums_ref[k, start : start + ROWS, :], axis=1, keepdims=True)
            spread = jnp.where(on_tile == tile, added, spread)
        return jnp.sum(jnp.where(on_row, spread, 0.0), axis=0, keepdims=True)

    norms = [jnp.zeros((1, LANES), jnp.float32)] * 3
    for first in range(0, residual_ref.shape[1], LANES):
        lanes = slice(first, first + LANES)
        weight = total(3, first)
        for k in range(3):
            residual = residual_ref[k : k + 1, lanes]
            image = residual + (total(k, first) + weight * own_ref[k : k + 1, lanes])
            image_ref[k : k + 1, lanes] = image
            terms = (residual * residual, residual * image, image * image)
            norms = [norm + term for norm, term in zip(norms, terms)]
    norms_ref[...] = jnp.zeros_like(norms_ref)
    for k in range(3):
        norms_ref[k : k + 1, :] = norms[k]


def pair_call(blobs, lhs=None, base=None, ending=None):
    diagonal = lhs is None
    wide = blobs.shape[1]
    own = wide if diagonal else lhs.shape[1]
    sub = max(64, 128 * 512 // wide)
    vmem = pl.BlockSpec(memory_space=pltpu.VMEM)
    sums = jax.ShapeDtypeStruct((4, own, LANES), jnp.float32)
    scratch = [pltpu.VMEM((DEPTH, wide), jnp.bfloat16)]
    scratch += [pltpu.VMEM((2 * sub, PIECE), jnp.float32)] * (wide // PIECE)
    pairs = own * wide
    aliases = {}
    if diagonal:
        args = [blobs]
        results = (sums, jax.ShapeDtypeStruct((2, own, DEPTH), jnp.bfloat16))
    elif ending is None:
        args = [blobs, lhs, base]
        results = (sums,)
        aliases = {2: 0}
    else:
        args = [blobs, lhs, base, *ending]
        results = (jax.ShapeDtypeStruct((3, own), jnp.float32), jax.ShapeDtypeStruct((ROWS, LANES), jnp.float32))
        scratch = [pltpu.VMEM(sums.shape, jnp.float32), *scratch]
    return pl.pallas_call(
        functools.partial(pair_kernel, diagonal, ending is not None),
        out_shape=results,
        in_specs=[vmem] * len(args),
        out_specs=(vmem,) * len(results),
        scratch_shapes=scratch,
        input_output_aliases=aliases,
        compiler_params=pltpu.CompilerParams(
            vmem_limit_bytes=16 << 20
        ),
        cost_estimate=pl.CostEstimate(flops=45 * pairs, bytes_accessed=32 * wide, transcendentals=pairs),
    )(*args)


WIDEST = 4096


def add_pairs(blobs, lhs, sums, ending=None):
    starts = range(0, blobs.shape[1], WIDEST)
    for first in starts[:-1]:
        (sums,) = pair_call(blobs[:, first : first + WIDEST], lhs, sums)
    return pair_call(blobs[:, starts[-1] :], lhs, sums, ending)


def update_kernel(mine_ref, other_ref, image_ref, residual_ref, iterate_ref, new_iterate_ref, new_residual_ref, new_direction_ref):
    norms = jnp.sum(mine_ref[...] + other_ref[...], axis=1, keepdims=True)
    old_norm, curvature, image_norm = norms[0:1], norms[1:2], norms[2:3]
    step_size = old_norm / curvature
    new_norm = old_norm - 2.0 * step_size * curvature + step_size * step_size * image_norm
    residual = residual_ref[...]
    new_residual = residual - step_size * image_ref[...]
    new_iterate_ref[...] = iterate_ref[...] + step_size * residual
    new_residual_ref[...] = new_residual
    new_direction_ref[...] = new_residual + new_norm / old_norm * residual


def update(mine, other, image, residual, iterate):
    vmem = pl.BlockSpec(memory_space=pltpu.VMEM)
    shape = jax.ShapeDtypeStruct(residual.shape, jnp.float32)
    return pl.pallas_call(
        update_kernel,
        out_shape=(shape,) * 3,
        in_specs=[vmem] * 5,
        out_specs=(vmem,) * 3,
        compiler_params=pltpu.CompilerParams(vmem_limit_bytes=4 << 20),
    )(mine, other, image, residual, iterate)


def strides(devices):
    out, step = [1], devices // 2
    while step > 1:
        out.append(step + 1)
        step //= 2
    return out


def swap(value, devices, step):
    return lax.ppermute(value, "tile", [(i, i ^ step) for i in range(devices)])


def shards(devices, positions, residual, iterate):
    one = jnp.ones((1, positions.shape[1]), jnp.float32)
    blobs = jnp.concatenate([STRETCH * (positions - CENTRE), one, FORCE * residual, one], axis=0)
    held, fresh, sums, lhs = blobs, blobs, None, None
    order = strides(devices)
    for step in order:
        arrived = swap(held, devices, step)
        if lhs is None:
            sums, lhs = pair_call(fresh)
        else:
            (sums,) = add_pairs(fresh, lhs, sums)
        sums, arrived = lax.optimization_barrier((sums, arrived))
        held = jnp.concatenate([held, arrived], axis=1)
        fresh = arrived
    image, norms = add_pairs(fresh, lhs, sums, (blobs, residual))
    other = jnp.zeros_like(norms)
    for step in order[1:] + order[:1]:
        norms = norms + other
        other = swap(norms, devices, step)
    return update(norms, other, image, residual, iterate)


def solution(mesh):
    spec = P("real", "tile")
    return jax.shard_map(
        functools.partial(shards, mesh.shape["tile"]),
        mesh=mesh,
        in_specs=(spec, spec, spec),
        out_specs=(spec, spec, spec),
        check_vma=False,
    )
```

```python
import functools

import jax
import jax.numpy as jnp
from jax import lax
from jax.experimental import pallas as pl
from jax.experimental.pallas import tpu as pltpu
from jax.sharding import PartitionSpec as P

LANES = 128
ROWS = 8
DEPTH = 128
CENTRE = 64.0
STRETCH = 1.5**0.5
FORCE = 0.75 * STRETCH
NEAR_SQ = 4.0 * 1.5
NEAR_CONST = 1.0 / FORCE
NEAR_SLOPE = 9.0 / (32.0 * STRETCH * FORCE)
NEAR_TENSOR = 1.0 / 36.0
FAR_AWAY = 1e30


def bf16(value):
    return value.astype(jnp.bfloat16).astype(jnp.float32)


def thirds(value):
    high = bf16(value)
    rest = value - high
    middle = bf16(rest)
    return high, middle, bf16(rest - middle)


def row_index(value):
    return lax.broadcasted_iota(jnp.int32, value.shape, 0)


def splits(blobs):
    row = row_index(blobs)
    place = row < 4
    tripled = jnp.where((row >= 4) & (row < 7), 3.0 * blobs, blobs)
    high = jnp.where(place, 0.5 * jnp.round(2.0 * blobs), bf16(tripled))
    rest = tripled - high
    middle = bf16(rest)
    low = bf16(rest - middle)
    return tripled, high, rest, middle, low


def column_features(blobs):
    row = row_index(blobs)
    tripled, high, rest, middle, low = splits(blobs)
    product = jnp.where(row < 4, high * high, tripled * pltpu.roll(blobs, 4, 0))
    p_high, p_middle, p_low = thirds(product)
    e_high, e_middle, e_low = thirds(rest * (2.0 * high + rest))
    zero = jnp.zeros_like(blobs)
    return [
        high, p_high, p_middle, high, high, middle, middle, middle,
        low, low, p_low, e_high, e_middle, e_low, zero, zero,
    ]


def row_features(blobs):
    row = row_index(blobs)
    place = row < 3
    _, high, rest, middle, low = splits(blobs)
    n_high, n_middle, n_low = thirds(jnp.sum(jnp.where(place, high * high, 0.0), axis=0, keepdims=True))
    fine = rest * (2.0 * high + rest)
    m_high, m_middle, m_low = thirds(jnp.sum(jnp.where(place, fine, 0.0), axis=0, keepdims=True))
    zero = jnp.zeros_like(blobs)
    one = jnp.where(place, 1.0, zero)

    def on(base, third, seventh):
        base = jnp.where(row == 3, third, jnp.where(place, base, 0.0))
        return jnp.where(row == 7, seventh, base)

    far = [
        on(-2.0 * high, n_high, n_middle), on(one, n_low, 0.0), one,
        on(-2.0 * middle, m_high, m_middle), on(-2.0 * low, m_low, 0.0),
        on(-2.0 * high, 0.0, 0.0), on(-2.0 * middle, 0.0, 0.0), on(-2.0 * low, 0.0, 0.0),
        on(-2.0 * high, 0.0, 0.0), on(-2.0 * middle, 0.0, 0.0),
        zero, one, one, one, zero, zero,
    ]

    def lift(value):
        return pltpu.roll(jnp.where(place, value, 0.0), 4, 0)

    big, mid, small, minus = lift(high), lift(middle), lift(low), lift(-one)
    along = [
        big, minus, minus, mid, small, big, mid, small,
        big, mid, minus, zero, zero, zero, zero, zero,
    ]
    return far, along


def pair_kernel(diagonal, last, *refs):
    if diagonal:
        blobs_ref, out_ref, lhs_ref, rhs_ref, *products_refs = refs
    elif last:
        blobs_ref, lhs_ref, base_ref, own_ref, residual_ref, image_ref, norms_ref, out_ref, rhs_ref, *products_refs = refs
    else:
        blobs_ref, lhs_ref, base_ref, out_ref, rhs_ref, *products_refs = refs
    own = lhs_ref.shape[1]
    cols = blobs_ref.shape[1] // LANES
    sub, width = products_refs[0].shape[0] // 2, products_refs[0].shape[1]
    steps = own // sub

    if diagonal:
        far, along = row_features(blobs_ref[...])
        lhs_ref[0] = jnp.concatenate(far, axis=0).T.astype(jnp.bfloat16)
        lhs_ref[1] = jnp.concatenate(along, axis=0).T.astype(jnp.bfloat16)

    def features(chunk):
        lanes = slice(chunk * own, (chunk + 1) * own)
        groups = column_features(blobs_ref[:, lanes])
        for pair in range(DEPTH // 16):
            both = jnp.concatenate(groups[2 * pair : 2 * pair + 2], axis=0)
            both = both.astype(jnp.bfloat16)
            for col in range(own // LANES):
                here = slice(col * LANES, (col + 1) * LANES)
                rhs_ref[chunk * own // LANES + col, 16 * pair : 16 * pair + 16, :] = both[:, here]

    def products(step, piece, into_refs):
        rows = pl.ds(pl.multiple_of(step * sub, sub), sub)
        first = piece * width // LANES
        columns = jnp.concatenate([rhs_ref[first + k] for k in range(width // LANES)], axis=1)
        both = jnp.concatenate([lhs_ref[0, rows, :], lhs_ref[1, rows, :]], axis=0)
        into_refs[piece][...] = jnp.dot(both, columns, preferred_element_type=jnp.float32)

    def add_column(step, col, acc, from_refs):
        first_row = pl.multiple_of(step * sub, sub)
        products_ref = from_refs[col * LANES // width]
        there = slice(col * LANES % width, col * LANES % width + LANES)
        lanes = slice(col * LANES, (col + 1) * LANES)
        x, y, z, fx, fy, fz = (
            jnp.broadcast_to(blobs_ref[k : k + 1, lanes], (ROWS, LANES)) for k in (0, 1, 2, 4, 5, 6)
        )
        for tile, mine in enumerate(acc):
            squared = products_ref[tile * ROWS : (tile + 1) * ROWS, there]
            projected = products_ref[sub + tile * ROWS : sub + (tile + 1) * ROWS, there]
            if diagonal:
                i = lax.broadcasted_iota(jnp.int32, (ROWS, LANES), 0) + (first_row + tile * ROWS)
                j = lax.broadcasted_iota(jnp.int32, (ROWS, LANES), 1) + col * LANES
                squared = jnp.where(i == j, FAR_AWAY, squared)
            inverse = lax.rsqrt(squared)
            limited = jnp.minimum(inverse * inverse, 1.0 / NEAR_SQ)
            cube = inverse * limited
            near_scalar = NEAR_CONST - NEAR_SLOPE * (squared * inverse)
            scalar = jnp.where(squared < NEAR_SQ, near_scalar, inverse + cube)
            weight = cube * (1.0 / 3.0 - limited) * projected
            mine[0] = mine[0] + (scalar * fx - weight * x)
            mine[1] = mine[1] + (scalar * fy - weight * y)
            mine[2] = mine[2] + (scalar * fz - weight * z)
            mine[3] = mine[3] + weight

    pieces = cols * LANES // width
    even_refs, odd_refs = products_refs[:pieces], products_refs[pieces:]
    for chunk in range(blobs_ref.shape[1] // own):
        features(chunk)
        for piece in range(chunk * own // width, (chunk + 1) * own // width):
            products(0, piece, even_refs)

    def add_step(step, from_refs, into_refs):
        later = jnp.minimum(step + 1, steps - 1)
        rows = [pl.ds(pl.multiple_of(step * sub, sub) + tile * ROWS, ROWS) for tile in range(sub // ROWS)]
        if diagonal:
            acc = [[jnp.zeros((ROWS, LANES), jnp.float32) for k in range(4)] for _ in rows]
        else:
            acc = [[base_ref[k, row, :] for k in range(4)] for row in rows]
        for group in range(pieces):
            for col in range(group * width // LANES, (group + 1) * width // LANES):
                add_column(step, col, acc, from_refs)
            products(later, group, into_refs)
        for row, mine in zip(rows, acc):
            for k in range(4):
                out_ref[k, row, :] = mine[k]

    def two_steps(turn, carry):
        add_step(2 * turn, even_refs, odd_refs)

        @pl.when(turn >= 0)
        def _():
            add_step(2 * turn + 1, odd_refs, even_refs)

        return carry

    lax.fori_loop(0, steps // 2, two_steps, 0)

    if last:
        finish(out_ref, own_ref, residual_ref, image_ref, norms_ref)


def finish(sums_ref, own_ref, residual_ref, image_ref, norms_ref):
    row = lax.broadcasted_iota(jnp.int32, (ROWS, LANES), 0)
    lane = lax.broadcasted_iota(jnp.int32, (ROWS, LANES), 1)
    on_row = row == lane % ROWS
    on_tile = lane // ROWS

    def total(k, first):
        spread = jnp.zeros((ROWS, LANES), jnp.float32)
        for tile in range(LANES // ROWS):
            start = first + tile * ROWS
            added = jnp.sum(sums_ref[k, start : start + ROWS, :], axis=1, keepdims=True)
            spread = jnp.where(on_tile == tile, added, spread)
        return jnp.sum(jnp.where(on_row, spread, 0.0), axis=0, keepdims=True)

    norms = [jnp.zeros((1, LANES), jnp.float32)] * 3
    for first in range(0, residual_ref.shape[1], LANES):
        lanes = slice(first, first + LANES)
        weight = total(3, first)
        for k in range(3):
            residual = residual_ref[k : k + 1, lanes]
            image = residual + (total(k, first) + weight * own_ref[k : k + 1, lanes])
            image_ref[k : k + 1, lanes] = image
            terms = (residual * residual, residual * image, image * image)
            norms = [norm + term for norm, term in zip(norms, terms)]
    norms_ref[...] = jnp.zeros_like(norms_ref)
    for k in range(3):
        norms_ref[k : k + 1, :] = norms[k]


def pair_call(blobs, lhs=None, base=None, ending=None):
    diagonal = lhs is None
    wide = blobs.shape[1]
    own = wide if diagonal else lhs.shape[1]
    sub = max(32, 256 * 512 // wide)
    vmem = pl.BlockSpec(memory_space=pltpu.VMEM)
    sums = jax.ShapeDtypeStruct((4, own, LANES), jnp.float32)
    scratch = [pltpu.VMEM((wide // LANES, DEPTH, LANES), jnp.bfloat16)]
    width = 256 if wide <= 1024 else 512
    scratch += [pltpu.VMEM((2 * sub, width), jnp.float32)] * (2 * wide // width)
    pairs = own * wide
    aliases = {}
    if diagonal:
        args = [blobs]
        results = (sums, jax.ShapeDtypeStruct((2, own, DEPTH), jnp.bfloat16))
    elif ending is None:
        args = [blobs, lhs, base]
        results = (sums,)
        aliases = {2: 0}
    else:
        args = [blobs, lhs, base, *ending]
        results = (jax.ShapeDtypeStruct((3, own), jnp.float32), jax.ShapeDtypeStruct((ROWS, LANES), jnp.float32))
        scratch = [pltpu.VMEM(sums.shape, jnp.float32), *scratch]
    return pl.pallas_call(
        functools.partial(pair_kernel, diagonal, ending is not None),
        out_shape=results,
        in_specs=[vmem] * len(args),
        out_specs=(vmem,) * len(results),
        scratch_shapes=scratch,
        input_output_aliases=aliases,
        compiler_params=pltpu.CompilerParams(
            vmem_limit_bytes=16 << 20
        ),
        cost_estimate=pl.CostEstimate(flops=45 * pairs, bytes_accessed=32 * wide, transcendentals=pairs),
    )(*args)


WIDEST = 4096


def add_pairs(blobs, lhs, sums, ending=None):
    starts = range(0, blobs.shape[1], WIDEST)
    for first in starts[:-1]:
        (sums,) = pair_call(blobs[:, first : first + WIDEST], lhs, sums)
    return pair_call(blobs[:, starts[-1] :], lhs, sums, ending)


def update_kernel(mine_ref, other_ref, image_ref, residual_ref, iterate_ref, new_iterate_ref, new_residual_ref, new_direction_ref):
    norms = jnp.sum(mine_ref[...] + other_ref[...], axis=1, keepdims=True)
    old_norm, curvature, image_norm = norms[0:1], norms[1:2], norms[2:3]
    step_size = old_norm / curvature
    new_norm = old_norm - 2.0 * step_size * curvature + step_size * step_size * image_norm
    residual = residual_ref[...]
    new_residual = residual - step_size * image_ref[...]
    new_iterate_ref[...] = iterate_ref[...] + step_size * residual
    new_residual_ref[...] = new_residual
    new_direction_ref[...] = new_residual + new_norm / old_norm * residual


def update(mine, other, image, residual, iterate):
    vmem = pl.BlockSpec(memory_space=pltpu.VMEM)
    shape = jax.ShapeDtypeStruct(residual.shape, jnp.float32)
    return pl.pallas_call(
        update_kernel,
        out_shape=(shape,) * 3,
        in_specs=[vmem] * 5,
        out_specs=(vmem,) * 3,
        compiler_params=pltpu.CompilerParams(vmem_limit_bytes=4 << 20),
    )(mine, other, image, residual, iterate)


def strides(devices):
    out, step = [1], devices // 2
    while step > 1:
        out.append(step + 1)
        step //= 2
    return out


def swap(value, devices, step):
    return lax.ppermute(value, "tile", [(i, i ^ step) for i in range(devices)])


def shards(devices, positions, residual, iterate):
    one = jnp.ones((1, positions.shape[1]), jnp.float32)
    blobs = jnp.concatenate([STRETCH * (positions - CENTRE), one, FORCE * residual, one], axis=0)
    held, fresh, sums, lhs = blobs, blobs, None, None
    order = strides(devices)
    for step in order:
        arrived = swap(held, devices, step)
        if lhs is None:
            sums, lhs = pair_call(fresh)
        else:
            (sums,) = add_pairs(fresh, lhs, sums)
        sums, arrived = lax.optimization_barrier((sums, arrived))
        held = jnp.concatenate([held, arrived], axis=1)
        fresh = arrived
    image, norms = add_pairs(fresh, lhs, sums, (blobs, residual))
    other = jnp.zeros_like(norms)
    for step in order[1:] + order[:1]:
        norms = norms + other
        other = swap(norms, devices, step)
    return update(norms, other, image, residual, iterate)


def solution(mesh):
    spec = P("real", "tile")
    return jax.shard_map(
        functools.partial(shards, mesh.shape["tile"]),
        mesh=mesh,
        in_specs=(spec, spec, spec),
        out_specs=(spec, spec, spec),
        check_vma=False,
    )
```

```python
import functools

import jax
import jax.numpy as jnp
from jax import lax
from jax.experimental import pallas as pl
from jax.experimental.pallas import tpu as pltpu
from jax.sharding import PartitionSpec as P

LANES = 128
ROWS = 8
DEPTH = 128
CENTRE = 64.0
STRETCH = 1.5**0.5
FORCE = 0.75 * STRETCH
NEAR_SQ = 4.0 * 1.5
NEAR_CONST = 1.0 / FORCE
NEAR_SLOPE = 9.0 / (32.0 * STRETCH * FORCE)
NEAR_TENSOR = 1.0 / 36.0
FAR_AWAY = 1e30


def bf16(value):
    return value.astype(jnp.bfloat16).astype(jnp.float32)


def thirds(value):
    high = bf16(value)
    rest = value - high
    middle = bf16(rest)
    return high, middle, bf16(rest - middle)


def row_index(value):
    return lax.broadcasted_iota(jnp.int32, value.shape, 0)


def splits(blobs):
    row = row_index(blobs)
    place = row < 4
    tripled = jnp.where((row >= 4) & (row < 7), 3.0 * blobs, blobs)
    high = jnp.where(place, 0.5 * jnp.round(2.0 * blobs), bf16(tripled))
    rest = tripled - high
    middle = bf16(rest)
    low = bf16(rest - middle)
    return tripled, high, rest, middle, low


def column_features(blobs):
    row = row_index(blobs)
    tripled, high, rest, middle, low = splits(blobs)
    product = jnp.where(row < 4, high * high, tripled * pltpu.roll(blobs, 4, 0))
    p_high, p_middle, p_low = thirds(product)
    e_high, e_middle, e_low = thirds(rest * (2.0 * high + rest))
    zero = jnp.zeros_like(blobs)
    return [
        high, p_high, p_middle, high, high, middle, middle, middle,
        low, low, p_low, e_high, e_middle, e_low, zero, zero,
    ]


def row_features(blobs):
    row = row_index(blobs)
    place = row < 3
    _, high, rest, middle, low = splits(blobs)
    n_high, n_middle, n_low = thirds(jnp.sum(jnp.where(place, high * high, 0.0), axis=0, keepdims=True))
    fine = rest * (2.0 * high + rest)
    m_high, m_middle, m_low = thirds(jnp.sum(jnp.where(place, fine, 0.0), axis=0, keepdims=True))
    zero = jnp.zeros_like(blobs)
    one = jnp.where(place, 1.0, zero)

    def on(base, third, seventh):
        base = jnp.where(row == 3, third, jnp.where(place, base, 0.0))
        return jnp.where(row == 7, seventh, base)

    far = [
        on(-2.0 * high, n_high, n_middle), on(one, n_low, 0.0), one,
        on(-2.0 * middle, m_high, m_middle), on(-2.0 * low, m_low, 0.0),
        on(-2.0 * high, 0.0, 0.0), on(-2.0 * middle, 0.0, 0.0), on(-2.0 * low, 0.0, 0.0),
        on(-2.0 * high, 0.0, 0.0), on(-2.0 * middle, 0.0, 0.0),
        zero, one, one, one, zero, zero,
    ]

    def lift(value):
        return pltpu.roll(jnp.where(place, value, 0.0), 4, 0)

    big, mid, small, minus = lift(high), lift(middle), lift(low), lift(-one)
    along = [
        big, minus, minus, mid, small, big, mid, small,
        big, mid, minus, zero, zero, zero, zero, zero,
    ]
    return far, along


def pair_kernel(diagonal, last, *refs):
    if diagonal:
        blobs_ref, out_ref, lhs_ref, rhs_ref, *products_refs = refs
    elif last:
        blobs_ref, lhs_ref, base_ref, own_ref, residual_ref, image_ref, norms_ref, out_ref, rhs_ref, *products_refs = refs
    else:
        blobs_ref, lhs_ref, base_ref, out_ref, rhs_ref, *products_refs = refs
    own = lhs_ref.shape[1]
    cols = blobs_ref.shape[1] // LANES
    sub, width = products_refs[0].shape[0] // 2, products_refs[0].shape[1]
    steps = own // sub

    if diagonal:
        far, along = row_features(blobs_ref[...])
        lhs_ref[0] = jnp.concatenate(far, axis=0).T.astype(jnp.bfloat16)
        lhs_ref[1] = jnp.concatenate(along, axis=0).T.astype(jnp.bfloat16)

    def features(chunk):
        lanes = slice(chunk * own, (chunk + 1) * own)
        groups = column_features(blobs_ref[:, lanes])
        for pair in range(DEPTH // 16):
            both = jnp.concatenate(groups[2 * pair : 2 * pair + 2], axis=0)
            both = both.astype(jnp.bfloat16)
            for col in range(own // LANES):
                here = slice(col * LANES, (col + 1) * LANES)
                rhs_ref[chunk * own // LANES + col, 16 * pair : 16 * pair + 16, :] = both[:, here]

    def products(step, piece, into_refs):
        rows = pl.ds(pl.multiple_of(step * sub, sub), sub)
        first = piece * width // LANES
        columns = jnp.concatenate([rhs_ref[first + k] for k in range(width // LANES)], axis=1)
        both = jnp.concatenate([lhs_ref[0, rows, :], lhs_ref[1, rows, :]], axis=0)
        into_refs[piece][...] = jnp.dot(both, columns, preferred_element_type=jnp.float32)

    def add_column(step, col, acc, from_refs):
        first_row = pl.multiple_of(step * sub, sub)
        products_ref = from_refs[col * LANES // width]
        there = slice(col * LANES % width, col * LANES % width + LANES)
        lanes = slice(col * LANES, (col + 1) * LANES)
        x, y, z, fx, fy, fz = (
            jnp.broadcast_to(blobs_ref[k : k + 1, lanes], (ROWS, LANES)) for k in (0, 1, 2, 4, 5, 6)
        )
        for tile, mine in enumerate(acc):
            squared = products_ref[tile * ROWS : (tile + 1) * ROWS, there]
            projected = products_ref[sub + tile * ROWS : sub + (tile + 1) * ROWS, there]
            if diagonal:
                i = lax.broadcasted_iota(jnp.int32, (ROWS, LANES), 0) + (first_row + tile * ROWS)
                j = lax.broadcasted_iota(jnp.int32, (ROWS, LANES), 1) + col * LANES
                squared = jnp.where(i == j, FAR_AWAY, squared)
            inverse = lax.rsqrt(squared)
            limited = jnp.minimum(inverse * inverse, 1.0 / NEAR_SQ)
            cube = inverse * limited
            near_scalar = NEAR_CONST - NEAR_SLOPE * (squared * inverse)
            scalar = jnp.where(squared < NEAR_SQ, near_scalar, inverse + cube)
            weight = cube * (1.0 / 3.0 - limited) * projected
            mine[0] = mine[0] + (scalar * fx - weight * x)
            mine[1] = mine[1] + (scalar * fy - weight * y)
            mine[2] = mine[2] + (scalar * fz - weight * z)
            mine[3] = mine[3] + weight

    pieces = cols * LANES // width
    even_refs, odd_refs = products_refs[:pieces], products_refs[pieces:]
    for chunk in range(blobs_ref.shape[1] // own):
        features(chunk)
        for piece in range(chunk * own // width, (chunk + 1) * own // width):
            products(0, piece, even_refs)

    def add_step(step, from_refs, into_refs):
        later = jnp.minimum(step + 1, steps - 1)
        rows = [pl.ds(pl.multiple_of(step * sub, sub) + tile * ROWS, ROWS) for tile in range(sub // ROWS)]
        if diagonal:
            acc = [[jnp.zeros((ROWS, LANES), jnp.float32) for k in range(4)] for _ in rows]
        else:
            acc = [[base_ref[k, row, :] for k in range(4)] for row in rows]
        for group in range(pieces):
            for col in range(group * width // LANES, (group + 1) * width // LANES):
                add_column(step, col, acc, from_refs)
            products(later, group, into_refs)
        for row, mine in zip(rows, acc):
            for k in range(4):
                out_ref[k, row, :] = mine[k]

    def two_steps(turn, carry):
        add_step(2 * turn, even_refs, odd_refs)

        @pl.when(turn >= 0)
        def _():
            add_step(2 * turn + 1, odd_refs, even_refs)

        return carry

    lax.fori_loop(0, steps // 2, two_steps, 0)

    if last:
        finish(out_ref, own_ref, residual_ref, image_ref, norms_ref)


def finish(sums_ref, own_ref, residual_ref, image_ref, norms_ref):
    row = lax.broadcasted_iota(jnp.int32, (ROWS, LANES), 0)
    lane = lax.broadcasted_iota(jnp.int32, (ROWS, LANES), 1)
    on_row = row == lane % ROWS
    on_tile = lane // ROWS

    def total(k, first):
        spread = jnp.zeros((ROWS, LANES), jnp.float32)
        for tile in range(LANES // ROWS):
            start = first + tile * ROWS
            added = jnp.sum(sums_ref[k, start : start + ROWS, :], axis=1, keepdims=True)
            spread = jnp.where(on_tile == tile, added, spread)
        return jnp.sum(jnp.where(on_row, spread, 0.0), axis=0, keepdims=True)

    norms = [jnp.zeros((1, LANES), jnp.float32)] * 3
    for first in range(0, residual_ref.shape[1], LANES):
        lanes = slice(first, first + LANES)
        weight = total(3, first)
        for k in range(3):
            residual = residual_ref[k : k + 1, lanes]
            image = residual + (total(k, first) + weight * own_ref[k : k + 1, lanes])
            image_ref[k : k + 1, lanes] = image
            terms = (residual * residual, residual * image, image * image)
            norms = [norm + term for norm, term in zip(norms, terms)]
    norms_ref[...] = jnp.zeros_like(norms_ref)
    for k in range(3):
        norms_ref[k : k + 1, :] = norms[k]


def pair_call(blobs, lhs=None, base=None, ending=None):
    diagonal = lhs is None
    wide = blobs.shape[1]
    own = wide if diagonal else lhs.shape[1]
    sub = max(32, 256 * 512 // wide)
    vmem = pl.BlockSpec(memory_space=pltpu.VMEM)
    sums = jax.ShapeDtypeStruct((4, own, LANES), jnp.float32)
    scratch = [pltpu.VMEM((wide // LANES, DEPTH, LANES), jnp.bfloat16)]
    width = 256 if wide <= 1024 else 512
    scratch += [pltpu.VMEM((2 * sub, width), jnp.float32)] * (2 * wide // width)
    pairs = own * wide
    aliases = {}
    if diagonal:
        args = [blobs]
        results = (sums, jax.ShapeDtypeStruct((2, own, DEPTH), jnp.bfloat16))
    elif ending is None:
        args = [blobs, lhs, base]
        results = (sums,)
        aliases = {2: 0}
    else:
        args = [blobs, lhs, base, *ending]
        results = (jax.ShapeDtypeStruct((3, own), jnp.float32), jax.ShapeDtypeStruct((ROWS, LANES), jnp.float32))
        scratch = [pltpu.VMEM(sums.shape, jnp.float32), *scratch]
    return pl.pallas_call(
        functools.partial(pair_kernel, diagonal, ending is not None),
        out_shape=results,
        in_specs=[vmem] * len(args),
        out_specs=(vmem,) * len(results),
        scratch_shapes=scratch,
        input_output_aliases=aliases,
        compiler_params=pltpu.CompilerParams(
            vmem_limit_bytes=16 << 20
        ),
        cost_estimate=pl.CostEstimate(flops=45 * pairs, bytes_accessed=32 * wide, transcendentals=pairs),
    )(*args)


WIDEST = 4096


def add_pairs(blobs, lhs, sums, ending=None):
    starts = range(0, blobs.shape[1], WIDEST)
    for first in starts[:-1]:
        (sums,) = pair_call(blobs[:, first : first + WIDEST], lhs, sums)
    return pair_call(blobs[:, starts[-1] :], lhs, sums, ending)


def update_kernel(mine_ref, other_ref, image_ref, residual_ref, iterate_ref, new_iterate_ref, new_residual_ref, new_direction_ref):
    norms = jnp.sum(mine_ref[...] + other_ref[...], axis=1, keepdims=True)
    old_norm, curvature, image_norm = norms[0:1], norms[1:2], norms[2:3]
    step_size = old_norm / curvature
    new_norm = old_norm - 2.0 * step_size * curvature + step_size * step_size * image_norm
    residual = residual_ref[...]
    new_residual = residual - step_size * image_ref[...]
    new_iterate_ref[...] = iterate_ref[...] + step_size * residual
    new_residual_ref[...] = new_residual
    new_direction_ref[...] = new_residual + new_norm / old_norm * residual


def update(mine, other, image, residual, iterate):
    vmem = pl.BlockSpec(memory_space=pltpu.VMEM)
    shape = jax.ShapeDtypeStruct(residual.shape, jnp.float32)
    return pl.pallas_call(
        update_kernel,
        out_shape=(shape,) * 3,
        in_specs=[vmem] * 5,
        out_specs=(vmem,) * 3,
        compiler_params=pltpu.CompilerParams(vmem_limit_bytes=4 << 20),
    )(mine, other, image, residual, iterate)


def strides(devices):
    out, step = [1], devices // 2
    while step > 1:
        out.append(step + 1)
        step //= 2
    return out


def swap(value, devices, step):
    return lax.ppermute(value, "tile", [(i, i ^ step) for i in range(devices)])


def shards(devices, positions, residual, iterate):
    one = jnp.ones((1, positions.shape[1]), jnp.float32)
    blobs = jnp.concatenate([STRETCH * (positions - CENTRE), one, FORCE * residual, one], axis=0)
    held, fresh, sums, lhs = blobs, blobs, None, None
    order = strides(devices)
    for turn, step in enumerate(order):
        arrived = swap(held, devices, step)
        if turn == 0 and len(order) > 1:
            blobs, arrived = lax.optimization_barrier((blobs, arrived))
            held, fresh = jnp.concatenate([blobs, arrived], axis=1), arrived
            continue
        if lhs is None:
            sums, lhs = pair_call(blobs)
        if turn > 0:
            (sums,) = add_pairs(fresh, lhs, sums)
        sums, arrived = lax.optimization_barrier((sums, arrived))
        held = jnp.concatenate([held, arrived], axis=1)
        fresh = arrived
    image, norms = add_pairs(fresh, lhs, sums, (blobs, residual))
    other = jnp.zeros_like(norms)
    for step in order[1:] + order[:1]:
        norms = norms + other
        other = swap(norms, devices, step)
    return update(norms, other, image, residual, iterate)


def solution(mesh):
    spec = P("real", "tile")
    return jax.shard_map(
        functools.partial(shards, mesh.shape["tile"]),
        mesh=mesh,
        in_specs=(spec, spec, spec),
        out_specs=(spec, spec, spec),
        check_vma=False,
    )
```
